32 devices in a mesh: ta: 4 (over z), gz: 2 (over x), xy: 4 (over y, core).
Axes of the slice: x: 2, y: 2, z: 4, core: 2. Of those that a mesh axis runs over, the one named last changes fastest.
Arguments:
- links: float32 [4, 2, 4, 4, 9, 4608], P('ta', 'gz', 'xy'), may hold values from -1 to 3
- eigvecs: float32 [4, 2, 4, 4, 48, 128], P('ta', 'gz', 'xy'), may hold values from -1 to 1
- eig_real: float32 [64], replicated, may hold values from 0.8 to 2.5
- eig_imag: float32 [64], replicated, may hold values from -0.5 to 0.5
- rhs: float32 [4, 2, 4, 4, 48, 128], P('ta', 'gz', 'xy'), may hold values from -3000 to 3000
Outputs:
- solution: float32 [4, 2, 4, 4, 48, 128], P('ta', 'gz', 'xy')
- residual: float32 [4, 2, 4, 4, 48, 128], P('ta', 'gz', 'xy')
The draws below stay inside these ranges and needn't reach their ends.
All inputs are finite; a program needn't handle non-finite values.
Results may differ from the reference program's by a relative error of at most 0.0003.
Values sent between devices are 32-bit elements; how exact they have to be, the bound alone decides.
A program may use at most 64 MiB of HBM per device.

```python
import jax
import jax.numpy as jnp
from jax import lax

DOF = 48
NEV = 64
NRHS = 64
SWEEPS = 4
NT = 4
NZ = 2
NX = 4
NY = 4


def eigen_fields(key):
    shape = (NT, NZ, NX, NY, DOF, 2 * NEV)
    values = jnp.clip(jax.random.normal(key, shape, jnp.float32), -4.0, 4.0)
    return values / jnp.sqrt(jnp.float32(NT * NZ * NX * NY * DOF * 2))


def draw_eigvecs(key, part):
    return eigen_fields(jax.random.fold_in(key, 7))


def draw_rhs(key, part):
    vectors = eigen_fields(jax.random.fold_in(key, 7))
    keys = jax.random.split(jax.random.fold_in(key, 13), 4)
    spread = jnp.sqrt(jnp.float32(NT * NZ * NX * NY * DOF * 2) / jnp.float32(2 * NEV))
    weights = jnp.clip(jax.random.normal(keys[0], (2 * NEV, NRHS), jnp.float32), -4.0, 4.0) * spread
    w_re = weights[:NEV]
    w_im = weights[NEV:]
    block = jnp.concatenate([jnp.concatenate([w_re, w_im], 1), jnp.concatenate([-w_im, w_re], 1)], 0)
    along = jnp.einsum('tzxydk,kc->tzxydc', vectors, block, precision=lax.Precision.HIGHEST)
    site_scale = jnp.exp(jax.random.uniform(keys[1], (NT, NZ, NX, NY, 1, 1), jnp.float32, 0.0, 2.3026))
    column = jnp.exp(jax.random.uniform(keys[2], (NRHS,), jnp.float32, 0.0, 2.3026))
    column = jnp.concatenate([column, column])
    ramp_t = 3.0 ** (jnp.arange(NT, dtype=jnp.float32) / max(NT - 1, 1))
    ramp_z = 3.0 ** (jnp.arange(NZ, dtype=jnp.float32) / max(NZ - 1, 1))
    ramp_x = 3.0 ** (jnp.arange(NX, dtype=jnp.float32) / max(NX - 1, 1))
    ramp = ramp_t[:, None, None] * ramp_z[None, :, None] * ramp_x[None, None, :]
    ramp = ramp[:, :, :, None, None, None]
    shape = (NT, NZ, NX, NY, DOF, 2 * NRHS)
    noise = jnp.clip(jax.random.normal(keys[3], shape, jnp.float32), -4.0, 4.0)
    return along + noise * site_scale * column * ramp / 30.0


def draw_links(key, part):
    keys = jax.random.split(jax.random.fold_in(key, 21), 2)
    shape = (NT, NZ, NX, NY, 9, DOF, 2 * DOF)
    noise = jnp.clip(jax.random.normal(keys[0], shape, jnp.float32), -4.0, 4.0)
    own = (jnp.arange(9) == 0).astype(jnp.float32)
    factor = 0.01 + 0.01 * own
    noise = noise * factor[:, None, None]
    mass = jax.random.uniform(keys[1], (NT, NZ, NX, NY, 1, 1, 1), jnp.float32, 1.0, 2.5)
    identity = jnp.eye(DOF, 2 * DOF, dtype=jnp.float32)
    full = noise + mass * identity[None, :, :] * own[:, None, None]
    return full.reshape(NT, NZ, NX, NY, 9, 2 * DOF * DOF)


def setup_inputs(seed: int = 0) -> dict:
    streams_of = jax.random.split(jax.random.key(seed), 6)
    links = draw_links(jax.random.fold_in(streams_of[5], 71), 0)
    eigvecs = draw_eigvecs(jax.random.fold_in(streams_of[5], 71), 0)
    eig_real = jnp.clip(jax.random.uniform(streams_of[2], (NEV,), jnp.float32, 0.8, 2.5), 0.8, 2.5)
    eig_imag = jnp.clip(jax.random.uniform(streams_of[3], (NEV,), jnp.float32, -0.5, 0.5), -0.5, 0.5)
    rhs = draw_rhs(jax.random.fold_in(streams_of[5], 71), 0)
    return {"links": links, "eigvecs": eigvecs, "eig_real": eig_real, "eig_imag": eig_imag, "rhs": rhs}


HIGH = lax.Precision.HIGHEST


def link_apply(matrix, field):
    half = field.shape[-1] // 2
    real = jnp.einsum('tzxyoi,tzxyic->tzxyoc', matrix[..., :DOF], field, precision=HIGH)
    imag = jnp.einsum('tzxyoi,tzxyic->tzxyoc', matrix[..., DOF:], field, precision=HIGH)
    return jnp.concatenate([real[..., :half] - imag[..., half:], real[..., half:] + imag[..., :half]], -1)


def operate(links, field):
    total = link_apply(links[:, :, :, :, 0], field)
    for axis in range(4):
        total = total - link_apply(links[:, :, :, :, 1 + axis], jnp.roll(field, -1, axis))
        total = total - link_apply(links[:, :, :, :, 5 + axis], jnp.roll(field, 1, axis))
    return total


def complex_scale(alpha_re, alpha_im, field):
    half = field.shape[-1] // 2
    f_re = field[..., :half]
    f_im = field[..., half:]
    return jnp.concatenate([alpha_re * f_re - alpha_im * f_im, alpha_re * f_im + alpha_im * f_re], -1)


def reference(links, eigvecs, eig_real, eig_imag, rhs):
    links = links.reshape(NT, NZ, NX, NY, 9, DOF, 2 * DOF)
    rows = eigvecs.reshape(-1, 2 * NEV)
    cross = jnp.dot(rows.T, rhs.reshape(-1, 2 * NRHS), precision=HIGH, preferred_element_type=jnp.float32)
    proj_re = cross[:NEV, :NRHS] + cross[NEV:, NRHS:]
    proj_im = cross[:NEV, NRHS:] - cross[NEV:, :NRHS]
    denom = (eig_real * eig_real + eig_imag * eig_imag)[:, None]
    coef_re = (proj_re * eig_real[:, None] + proj_im * eig_imag[:, None]) / denom
    coef_im = (proj_im * eig_real[:, None] - proj_re * eig_imag[:, None]) / denom
    block = jnp.concatenate([jnp.concatenate([coef_re, coef_im], 1), jnp.concatenate([-coef_im, coef_re], 1)], 0)
    solution = jnp.dot(rows, block, precision=HIGH, preferred_element_type=jnp.float32).reshape(rhs.shape)
    residual = rhs - operate(links, solution)
    for sweep in range(SWEEPS):
        image = operate(links, residual)
        swapped = jnp.concatenate([residual[..., NRHS:], residual[..., :NRHS]], -1)
        first = jnp.sum(image * residual, axis=(0, 1, 2, 3, 4))
        second = jnp.sum(image * swapped, axis=(0, 1, 2, 3, 4))
        power = jnp.sum(image * image, axis=(0, 1, 2, 3, 4))
        num_re = first[:NRHS] + first[NRHS:]
        num_im = second[:NRHS] - second[NRHS:]
        den = power[:NRHS] + power[NRHS:]
        alpha_re = num_re / den
        alpha_im = num_im / den
        solution = solution + complex_scale(alpha_re, alpha_im, residual)
        residual = residual - complex_scale(alpha_re, alpha_im, image)
    return solution, residual
```

```python
import functools

import jax
import jax.numpy as jnp
from jax import lax
from jax.experimental import pallas as pl
from jax.experimental.pallas import tpu as pltpu
from jax.sharding import PartitionSpec as P

SWEEPS = 4
HIGH = lax.Precision.HIGHEST
MESH = pl.DeviceIdType.MESH
F32, BF16 = jnp.float32, jnp.bfloat16


def split(x):
    first = x.astype(BF16)
    x = x - first.astype(F32)
    second = x.astype(BF16)
    return first, second, (x - second.astype(F32)).astype(BF16)


def kernel(
    sizes, dims, links_hbm, v_ref, er_ref, ei_ref, rhs_ref, sol_ref, res_ref,
    links, tail, flat, mats, srcs, acc, fields, halos, w_ref, cfull, cpart, rs_buf, ct_buf,
    ag_buf, at_buf, ap_buf, vw,
    link_sem, halo_send, halo_recv, rs_send, rs_recv, ct_send, ct_recv, ag_send, ag_recv,
    at_send, at_recv, ap_send, ap_recv,
):
    nt, nz, nx = sizes
    ny, dof, lanes = dims
    half = lanes // 2
    plane = nz * nx
    it, iz, ix = lax.axis_index("ta"), lax.axis_index("gz"), lax.axis_index("xy")
    me = iz * nx + ix

    link_copy = pltpu.make_async_copy(links_hbm, links, link_sem)
    link_copy.start()

    def plane_peer(k):
        p = lax.rem(me + k, plane)
        return p, {"ta": it, "gz": lax.div(p, nx), "xy": lax.rem(p, nx)}

    def time_peer(k):
        p = lax.rem(it + k, nt)
        return p, {"ta": p, "gz": iz, "xy": ix}

    barrier = pltpu.get_barrier_semaphore()
    for k in range(1, plane):
        pl.semaphore_signal(barrier, inc=1, device_id=plane_peer(k)[1], device_id_type=MESH)
    for k in range(1, nt):
        pl.semaphore_signal(barrier, inc=1, device_id=time_peer(k)[1], device_id_type=MESH)

    def neighbours(axis, index, n):
        base = {"ta": it, "gz": iz, "xy": ix}
        up, down = dict(base), dict(base)
        up[axis] = lax.rem(index + 1, n)
        down[axis] = lax.rem(index + n - 1, n)
        return up, down

    outgoing, groups, slot = [], {}, 0
    for axis, index, n, d in (("ta", it, nt, 1), ("xy", ix, nx, 3), ("gz", iz, nz, 2)):
        up, down = neighbours(axis, index, n)
        if n == 2:
            outgoing.append((slot, up))
            groups[axis] = [(slot, (d, d + 4))]
            slot += 1
        else:
            outgoing.append((slot, down))
            outgoing.append((slot + 1, up))
            groups[axis] = [(slot, (d,)), (slot + 1, (d + 4,))]
            slot += 2
    far, near = groups["ta"], groups["xy"] + groups["gz"]

    def send_field(rnd, src):
        out = []
        for s, target in outgoing:
            c = pltpu.make_async_remote_copy(
                src_ref=src, dst_ref=halos.at[rnd, s],
                send_sem=halo_send.at[rnd, s], recv_sem=halo_recv.at[rnd, s],
                device_id=target, device_id_type=MESH,
            )
            c.start()
            out.append((s, c))
        return dict(out)

    def share(buf, mine, n, peer, send, recv):
        out = []
        for k in range(1, n):
            c = pltpu.make_async_remote_copy(
                src_ref=buf.at[mine], dst_ref=buf.at[mine],
                send_sem=send.at[k], recv_sem=recv.at[k],
                device_id=peer(k)[1], device_id_type=MESH,
            )
            c.start()
            out.append(c)
        return out

    def recv_all(copies):
        for c in copies:
            c.wait_recv()

    lane = lax.broadcasted_iota(jnp.int32, (1, lanes), 1)
    low = lane < half
    jsign = jnp.where(low, -1.0, 1.0).astype(F32)

    def swap(x):
        return pltpu.roll(x, half, 1)

    pl.semaphore_wait(barrier, plane - 1 + nt - 1)

    sends = []
    v_copies = send_field(0, v_ref)
    sends += list(v_copies.values())

    rows = v_ref[...].reshape(ny * dof, lanes)
    cross = lax.dot_general(
        rows, rhs_ref[...].reshape(ny * dof, lanes), (((0,), (0,)), ((), ())),
        precision=HIGH, preferred_element_type=F32,
    )
    cfull[...] = cross[:half] - jsign * swap(cross[half:])
    part = half // plane
    for p in range(plane):
        cpart[p] = cfull[p * part : (p + 1) * part]
    rs_copies = []
    for k in range(1, plane):
        p, target = plane_peer(k)
        c = pltpu.make_async_remote_copy(
            src_ref=cpart.at[p], dst_ref=rs_buf.at[me],
            send_sem=rs_send.at[k], recv_sem=rs_recv.at[k],
            device_id=target, device_id_type=MESH,
        )
        c.start()
        rs_copies.append(c)
    rs_buf[me] = cpart[me]
    sends += rs_copies

    link_copy.wait()
    tail[...] = jnp.zeros_like(tail)
    for y in range(ny):
        tail[pl.ds(y, 1), :] = links[y, 8:9, :]
    two = 2 * dof
    valid = lane < two

    def pick(ref_load, b, j):
        at = j * two
        base, off = (at // 128) * 128, at % 128
        start = pl.multiple_of(b * (4 * two), 128) + base
        width = 128 if off + two <= 128 else 256
        x = ref_load(pl.ds(start, width))
        if off:
            x = pltpu.roll(x, width - off, 1)
        return jnp.where(valid, x[:, :128], 0.0)

    def relayout(b, carry):
        for g in range(ny + 1):
            load = (lambda w, g=g: links[g, 0:8, w]) if g < ny else (lambda w: tail[:, w])
            for j in range(4):
                flat[pl.ds(g * 8 * dof + 4 * b + j, 8, stride=dof), :] = pick(load, b, j)
        return carry

    lax.fori_loop(0, dof // 4, relayout, 0)

    def direction(y, d):
        r = (y * 8 + d) * dof if d < 8 else (ny * 8 + y) * dof
        return flat[pl.ds(r, dof), :]

    order = [(0,), (4,), (8,)] + [ds for _, ds in near] + [ds for _, ds in far]
    for y in range(ny):
        for m, ds in enumerate(order):
            x = direction(y, ds[0])
            for d in ds[1:]:
                x = x + direction(y, d)
            if ds[0]:
                x = -x
            for i, piece in enumerate(split(x)):
                mats[y, i * dof : (i + 1) * dof, m * 128 : (m + 1) * 128] = piece
    srcs[:, :, two:, :] = jnp.zeros((srcs.shape[0], ny, srcs.shape[2] - two, 3 * lanes), BF16)

    def prepare(m, y, x):
        for i, piece in enumerate(split(x)):
            srcs[m, y, :dof, i * lanes : (i + 1) * lanes] = piece
        for i, piece in enumerate(split(swap(x) * jsign)):
            srcs[m, y, dof:two, i * lanes : (i + 1) * lanes] = piece

    def product(y, m0, blocks):
        right = jnp.concatenate([srcs[s, z] for s, z in blocks], 0)
        left = mats[y, :, m0 * 128 : (m0 + len(blocks)) * 128]
        main = jnp.dot(left, right[:, : 2 * lanes], preferred_element_type=F32)
        small = jnp.dot(left[:dof], right[:, 2 * lanes :], preferred_element_type=F32)
        second = main[dof : 2 * dof]
        small = small + main[2 * dof :, :lanes] + second[:, lanes:]
        return main[:dof, :lanes] + (main[:dof, lanes:] + second[:, :lanes] + small)

    def begin(field):
        for y in range(ny):
            prepare(0, y, field[y])
        for y in range(ny):
            acc[y] = product(y, 0, [(0, y), (0, (y + 1) % ny), (0, (y - 1) % ny)])

    def middle(rnd, copies):
        for i, (s, _) in enumerate(near):
            copies[s].wait_recv()
            for y in range(ny):
                prepare(1 + i, y, halos[rnd, s, y])
        for y in range(ny):
            acc[y] += product(y, 3, [(1 + i, y) for i in range(len(near))])

    def finish(rnd, copies, emit):
        first = 1 + len(near)
        for i, (s, _) in enumerate(far):
            copies[s].wait_recv()
            for y in range(ny):
                prepare(first + i, y, halos[rnd, s, y])
        for y in range(ny):
            t = acc[y] + product(y, 3 + len(near), [(first + i, y) for i in range(len(far))])
            emit(y, t)

    recv_all(rs_copies)
    total = rs_buf[0]
    for p in range(1, plane):
        total = total + rs_buf[p]
    ct_buf[it] = total
    ct_copies = share(ct_buf, it, nt, time_peer, ct_send, ct_recv)
    sends += ct_copies

    begin(v_ref)

    recv_all(ct_copies)
    total = ct_buf[0]
    for p in range(1, nt):
        total = total + ct_buf[p]
    ag_buf[me] = total
    ag_copies = share(ag_buf, me, plane, plane_peer, ag_send, ag_recv)
    sends += ag_copies

    middle(0, v_copies)

    def keep(y, value):
        w_ref[y] = value

    finish(0, v_copies, keep)
    for i, ref in enumerate((v_ref, w_ref)):
        one, other, third = split(ref[...].reshape(ny * dof, lanes))
        for j, piece in enumerate((one, other, one, third)):
            vw[i * ny * dof : (i + 1) * ny * dof, j * lanes : (j + 1) * lanes] = piece

    recv_all(ag_copies)
    for p in range(plane):
        cfull[p * part : (p + 1) * part] = ag_buf[p]
    corr = cfull[...]
    eye = lax.broadcasted_iota(jnp.int32, (half, half), 0) == lax.broadcasted_iota(
        jnp.int32, (half, half), 1
    )
    er = jnp.sum(jnp.where(eye, er_ref[...], 0.0), axis=1, keepdims=True)
    ei = jnp.sum(jnp.where(eye, ei_ref[...], 0.0), axis=1, keepdims=True)
    coef = (corr * er - jsign * swap(corr) * ei) / (er * er + ei * ei)
    b1, b2, b3 = split(jnp.concatenate([coef, jsign * swap(coef)], 0))
    block = jnp.concatenate([b1, b2], 1)
    block = jnp.concatenate([block, block], 0)
    both = jnp.dot(vw[:, : 2 * lanes], block, preferred_element_type=F32)
    small = jnp.dot(
        vw[:, 2 * lanes :], jnp.concatenate([b3, b1], 0), preferred_element_type=F32
    )
    both = both[:, :lanes] + (both[:, lanes:] + small)
    n = ny * dof
    r0 = rhs_ref[...] - both[n:].reshape(ny, dof, lanes)
    fields[0] = r0
    copies = send_field(1, fields.at[0])
    sends += list(copies.values())
    sol_ref[...] = both[:n].reshape(ny, dof, lanes)
    res_ref[...] = r0

    begin(fields.at[0])
    middle(1, copies)

    def to_first(y, value):
        fields[1, y] = value

    finish(1, copies, to_first)

    for sweep in range(SWEEPS):
        image = fields.at[sweep + 1]
        last = sweep + 1 == SWEEPS
        s1 = jnp.zeros((1, lanes), F32)
        s2, s3 = s1, s1
        for y in range(ny):
            f, r = image[y], res_ref[y]
            s1 = s1 + jnp.sum(f * r, axis=0, keepdims=True)
            s2 = s2 + jnp.sum(f * swap(r), axis=0, keepdims=True)
            s3 = s3 + jnp.sum(f * f, axis=0, keepdims=True)
        num = jnp.where(low, s1 + swap(s1), swap(s2) - s2)
        den = s3 + swap(s3)
        row = lax.broadcasted_iota(jnp.int32, (8, lanes), 0)
        tbuf, pbuf = at_buf.at[sweep], ap_buf.at[sweep]
        tbuf[it] = jnp.where(row == 0, num, den)
        t_copies = share(tbuf, it, nt, time_peer, at_send.at[sweep], at_recv.at[sweep])
        sends += t_copies
        if not last:
            copies = send_field(sweep + 2, image)
            sends += list(copies.values())
            begin(image)
        recv_all(t_copies)
        total = tbuf[0]
        for p in range(1, nt):
            total = total + tbuf[p]
        pbuf[me] = total
        p_copies = share(pbuf, me, plane, plane_peer, ap_send.at[sweep], ap_recv.at[sweep])
        sends += p_copies
        if not last:
            middle(sweep + 2, copies)
        recv_all(p_copies)
        total = pbuf[0]
        for p in range(1, plane):
            total = total + pbuf[p]
        a = total[0:1] / total[1:2]
        sa = swap(a)
        ar = jnp.where(low, a, sa)
        ai = jnp.where(low, sa, a) * jsign
        for y in range(ny):
            f, r = image[y], res_ref[y]
            sol_ref[y] = sol_ref[y] + (ar * r + ai * swap(r))
            res_ref[y] = r - (ar * f + ai * swap(f))
        if not last:

            def update(y, value):
                fields[sweep + 2, y] = image[y] - (ar * value + ai * swap(value))

            finish(sweep + 2, copies, update)
    for c in sends:
        c.wait_send()


def local(sizes, links, eigvecs, eig_real, eig_imag, rhs):
    nt, nz, nx = sizes
    plane = nz * nx
    ny, dof, lanes = rhs.shape[3:]
    half = lanes // 2
    field = (ny, dof, lanes)
    ndir = links.shape[4]
    slots = sum(1 if n == 2 else 2 for n in sizes)
    part = half // plane
    rounds = SWEEPS + 1
    vmem, dma = pltpu.VMEM, pltpu.SemaphoreType.DMA
    spec = pl.BlockSpec(memory_space=pltpu.VMEM)
    sol, res = pl.pallas_call(
        functools.partial(kernel, sizes, field),
        out_shape=[jax.ShapeDtypeStruct(field, F32)] * 2,
        in_specs=[pl.BlockSpec(memory_space=pl.ANY)] + [spec] * 4,
        out_specs=[spec] * 2,
        scratch_shapes=[
            vmem((ny, ndir, links.shape[5]), F32),
            vmem((8, links.shape[5]), F32),
            vmem(((ny * 8 + 8) * dof, 128), F32),
            vmem((ny, 3 * dof, (3 + slots) * 128), BF16),
            vmem((1 + slots, ny, 128, 3 * lanes), BF16),
            vmem(field, F32),
            vmem((rounds,) + field, F32),
            vmem((rounds, slots) + field, F32),
            vmem(field, F32),
            vmem((half, lanes), F32),
            vmem((plane, part, lanes), F32),
            vmem((plane, part, lanes), F32),
            vmem((nt, part, lanes), F32),
            vmem((plane, part, lanes), F32),
            vmem((SWEEPS, nt, 8, lanes), F32),
            vmem((SWEEPS, plane, 8, lanes), F32),
            vmem((2 * ny * dof, 4 * lanes), BF16),
            dma,
            dma((rounds, slots)),
            dma((rounds, slots)),
            dma((plane,)),
            dma((plane,)),
            dma((nt,)),
            dma((nt,)),
            dma((plane,)),
            dma((plane,)),
            dma((SWEEPS, nt)),
            dma((SWEEPS, nt)),
            dma((SWEEPS, plane)),
            dma((SWEEPS, plane)),
        ],
        compiler_params=pltpu.CompilerParams(collective_id=0, has_side_effects=True),
    )(
        links.reshape(links.shape[3:]),
        eigvecs.reshape(field),
        eig_real.reshape(1, -1),
        eig_imag.reshape(1, -1),
        rhs.reshape(field),
    )
    return (sol.reshape(rhs.shape), res.reshape(rhs.shape))


def solution(mesh):
    whole = P("ta", "gz", "xy", None, None, None)
    sizes = tuple(mesh.shape[a] for a in ("ta", "gz", "xy"))
    return jax.shard_map(
        functools.partial(local, sizes),
        mesh=mesh,
        in_specs=(whole, whole, P(), P(), whole),
        out_specs=(whole, whole),
        check_vma=False,
    )
```

```python
import functools

import jax
import jax.numpy as jnp
from jax import lax
from jax.experimental import pallas as pl
from jax.experimental.pallas import tpu as pltpu
from jax.sharding import PartitionSpec as P

SWEEPS = 4
DIRECT = 32
HIGH = lax.Precision.HIGHEST
MESH = pl.DeviceIdType.MESH
F32, BF16 = jnp.float32, jnp.bfloat16


def split(x):
    first = x.astype(BF16)
    x = x - first.astype(F32)
    second = x.astype(BF16)
    return first, second, (x - second.astype(F32)).astype(BF16)


def kernel(
    sizes, dims, links_hbm, v_ref, er_ref, ei_ref, rhs_ref, sol_ref, res_ref,
    links, flat, mats, srcs, acc, fields, halos, w_ref, cfull, cpart, rs_buf, ct_buf,
    ag_buf, at_buf, ap_buf, vw,
    link_sem, halo_send, halo_recv, rs_send, rs_recv, ct_send, ct_recv, ag_send, ag_recv,
    at_send, at_recv, ap_send, ap_recv,
):
    nt, nz, nx = sizes
    ny, dof, lanes = dims
    half = lanes // 2
    plane = nz * nx
    it, iz, ix = lax.axis_index("ta"), lax.axis_index("gz"), lax.axis_index("xy")
    me = iz * nx + ix

    link_copy = pltpu.make_async_copy(links_hbm, links, link_sem)
    link_copy.start()

    def plane_peer(k):
        p = lax.rem(me + k, plane)
        return p, {"ta": it, "gz": lax.div(p, nx), "xy": lax.rem(p, nx)}

    def time_peer(k):
        p = lax.rem(it + k, nt)
        return p, {"ta": p, "gz": iz, "xy": ix}

    everyone = nt * plane
    rank = it * plane + me

    def any_peer(k):
        p = lax.rem(rank + k, everyone)
        r = lax.rem(p, plane)
        return p, {"ta": lax.div(p, plane), "gz": lax.div(r, nx), "xy": lax.rem(r, nx)}

    direct = everyone <= DIRECT
    if direct:
        greeted = [any_peer(k)[1] for k in range(1, everyone)]
    else:
        greeted = [plane_peer(k)[1] for k in range(1, plane)]
        greeted += [time_peer(k)[1] for k in range(1, nt)]
    barrier = pltpu.get_barrier_semaphore()
    for target in greeted:
        pl.semaphore_signal(barrier, inc=1, device_id=target, device_id_type=MESH)

    def neighbours(axis, index, n):
        base = {"ta": it, "gz": iz, "xy": ix}
        up, down = dict(base), dict(base)
        up[axis] = lax.rem(index + 1, n)
        down[axis] = lax.rem(index + n - 1, n)
        return up, down

    outgoing, groups, slot = [], {}, 0
    for axis, index, n, d in (("ta", it, nt, 1), ("xy", ix, nx, 3), ("gz", iz, nz, 2)):
        up, down = neighbours(axis, index, n)
        if n == 2:
            outgoing.append((axis, slot, up))
            groups[axis] = [(slot, (d, d + 4))]
            slot += 1
        else:
            turn = jnp.where(index == n - 1, 1, 0)
            for t in (turn, 1 - turn):
                target = dict(up)
                target[axis] = lax.rem(index + n - 1 + 2 * t, n)
                outgoing.append((axis, slot + t, target))
            groups[axis] = [(slot, (d,)), (slot + 1, (d + 4,))]
            slot += 2
    far, near = groups["ta"], groups["xy"] + groups["gz"]

    def send_field(rnd, src, axes=("ta", "xy", "gz")):
        out = []
        for axis, s, target in outgoing:
            if axis not in axes:
                continue
            c = pltpu.make_async_remote_copy(
                src_ref=src, dst_ref=halos.at[rnd, s],
                send_sem=halo_send.at[rnd, s], recv_sem=halo_recv.at[rnd, s],
                device_id=target, device_id_type=MESH,
            )
            c.start()
            out.append(c)
        return out

    def arrived(rnd, s):
        pltpu.make_async_remote_copy(
            src_ref=v_ref, dst_ref=halos.at[rnd, s],
            send_sem=halo_send.at[rnd, s], recv_sem=halo_recv.at[rnd, s],
            device_id=outgoing[0][2], device_id_type=MESH,
        ).wait_recv()

    def share(buf, mine, n, peer, send, recv):
        out = []
        for k in range(1, n):
            c = pltpu.make_async_remote_copy(
                src_ref=buf.at[mine], dst_ref=buf.at[mine],
                send_sem=send.at[k], recv_sem=recv.at[k],
                device_id=peer(k)[1], device_id_type=MESH,
            )
            c.start()
            out.append(c)
        return out

    def recv_all(copies):
        for c in copies:
            c.wait_recv()

    def add_slots(buf, n):
        parts = [buf[p] for p in range(n)]
        while len(parts) > 1:
            odd = parts[len(parts) // 2 * 2 :]
            parts = [a + b for a, b in zip(parts[::2], parts[1::2])] + odd
        return parts[0]

    lane = lax.broadcasted_iota(jnp.int32, (1, lanes), 1)
    low = lane < half
    jsign = jnp.where(low, -1.0, 1.0).astype(F32)

    def swap(x):
        return pltpu.roll(x, half, 1)

    sends = []
    rows = v_ref[...].reshape(ny * dof, lanes)
    cross = lax.dot_general(
        rows, rhs_ref[...].reshape(ny * dof, lanes), (((0,), (0,)), ((), ())),
        precision=HIGH, preferred_element_type=F32,
    )
    cfull[...] = cross[:half] - jsign * swap(cross[half:])
    part = half // plane
    for p in range(plane):
        cpart[p] = cfull[p * part : (p + 1) * part]
    pl.semaphore_wait(barrier, len(greeted))
    rs_copies = []
    for k in range(1, plane):
        p, target = plane_peer(k)
        c = pltpu.make_async_remote_copy(
            src_ref=cpart.at[p], dst_ref=rs_buf.at[me],
            send_sem=rs_send.at[k], recv_sem=rs_recv.at[k],
            device_id=target, device_id_type=MESH,
        )
        c.start()
        rs_copies.append(c)
    rs_buf[me] = cpart[me]
    sends += rs_copies
    sends += send_field(0, v_ref, ("xy", "gz"))

    link_copy.wait()
    two = 2 * dof
    valid = lane < two

    def pick(pair, b, j):
        at = j * two
        base, off = (at // 128) * 128, at % 128
        start = pl.multiple_of(b * (4 * two), 128) + base
        width = 128 if off + two <= 128 else 256
        x = [links[d, :, pl.ds(start, width)] for d in pair]
        x = jnp.concatenate(x, 0) if len(x) > 1 else x[0]
        if off:
            x = pltpu.roll(x, width - off, 1)
        return jnp.where(valid, x[:, :128], 0.0)

    def relayout(b, carry):
        for pair in ((0, 1), (2, 3), (4, 5), (6, 7), (8,)):
            for j in range(4):
                row = pair[0] * ny * dof + 4 * b + j
                flat[pl.ds(row, len(pair) * ny, stride=dof), :] = pick(pair, b, j)
        return carry

    lax.fori_loop(0, dof // 4, relayout, 0)

    def direction(y, d):
        return flat[pl.ds((d * ny + y) * dof, dof), :]

    order = [(0,), (4,), (8,)] + [ds for _, ds in near] + [ds for _, ds in far]
    for y in range(ny):
        for m, ds in enumerate(order):
            x = direction(y, ds[0])
            for d in ds[1:]:
                x = x + direction(y, d)
            if ds[0]:
                x = -x
            for i, piece in enumerate(split(x)):
                mats[y, i * dof : (i + 1) * dof, m * 128 : (m + 1) * 128] = piece
    srcs[:, :, two:, :] = jnp.zeros((srcs.shape[0], ny, srcs.shape[2] - two, 3 * lanes), BF16)

    def prepare(m, y, x):
        for i, piece in enumerate(split(x)):
            srcs[m, y, :dof, i * lanes : (i + 1) * lanes] = piece
        for i, piece in enumerate(split(swap(x) * jsign)):
            srcs[m, y, dof:two, i * lanes : (i + 1) * lanes] = piece

    def product(y, m0, blocks):
        right = jnp.concatenate([srcs[s, z] for s, z in blocks], 0)
        left = mats[y, :, m0 * 128 : (m0 + len(blocks)) * 128]
        main = jnp.dot(left, right[:, : 2 * lanes], preferred_element_type=F32)
        small = jnp.dot(left[:dof], right[:, 2 * lanes :], preferred_element_type=F32)
        second = main[dof : 2 * dof]
        small = small + main[2 * dof :, :lanes] + second[:, lanes:]
        return main[:dof, :lanes] + (main[:dof, lanes:] + second[:, :lanes] + small)

    def begin(field):
        for y in range(ny):
            prepare(0, y, field[y])
        for y in range(ny):
            acc[y] = product(y, 0, [(0, y), (0, (y + 1) % ny), (0, (y - 1) % ny)])

    def middle(rnd):
        for i, (s, _) in enumerate(near):
            arrived(rnd, s)
            for y in range(ny):
                prepare(1 + i, y, halos[rnd, s, y])
        for y in range(ny):
            acc[y] += product(y, 3, [(1 + i, y) for i in range(len(near))])

    def finish(rnd, emit):
        first = 1 + len(near)
        for i, (s, _) in enumerate(far):
            arrived(rnd, s)
            for y in range(ny):
                prepare(first + i, y, halos[rnd, s, y])
        for y in range(ny):
            t = acc[y] + product(y, 3 + len(near), [(first + i, y) for i in range(len(far))])
            emit(y, t)

    recv_all(rs_copies)
    total = rs_buf[0]
    for p in range(1, plane):
        total = total + rs_buf[p]
    ct_buf[it] = total
    ct_copies = share(ct_buf, it, nt, time_peer, ct_send, ct_recv)
    sends += ct_copies
    sends += send_field(0, v_ref, ("ta",))

    begin(v_ref)

    recv_all(ct_copies)
    total = ct_buf[0]
    for p in range(1, nt):
        total = total + ct_buf[p]
    ag_buf[me] = total
    ag_copies = share(ag_buf, me, plane, plane_peer, ag_send, ag_recv)
    sends += ag_copies

    middle(0)

    def keep(y, value):
        w_ref[y] = value

    finish(0, keep)
    for i, ref in enumerate((v_ref, w_ref)):
        one, other, third = split(ref[...].reshape(ny * dof, lanes))
        for j, piece in enumerate((one, other, one, third)):
            vw[i * ny * dof : (i + 1) * ny * dof, j * lanes : (j + 1) * lanes] = piece

    recv_all(ag_copies)
    for p in range(plane):
        cfull[p * part : (p + 1) * part] = ag_buf[p]
    corr = cfull[...]
    eye = lax.broadcasted_iota(jnp.int32, (half, half), 0) == lax.broadcasted_iota(
        jnp.int32, (half, half), 1
    )
    er = jnp.sum(jnp.where(eye, er_ref[...], 0.0), axis=1, keepdims=True)
    ei = jnp.sum(jnp.where(eye, ei_ref[...], 0.0), axis=1, keepdims=True)
    coef = (corr * er - jsign * swap(corr) * ei) / (er * er + ei * ei)
    b1, b2, b3 = split(jnp.concatenate([coef, jsign * swap(coef)], 0))
    block = jnp.concatenate([b1, b2], 1)
    block = jnp.concatenate([block, block], 0)
    both = jnp.dot(vw[:, : 2 * lanes], block, preferred_element_type=F32)
    small = jnp.dot(
        vw[:, 2 * lanes :], jnp.concatenate([b3, b1], 0), preferred_element_type=F32
    )
    both = both[:, :lanes] + (both[:, lanes:] + small)
    n = ny * dof
    r0 = rhs_ref[...] - both[n:].reshape(ny, dof, lanes)
    fields[0] = r0
    sends += send_field(1, fields.at[0])
    sol_ref[...] = both[:n].reshape(ny, dof, lanes)
    res_ref[...] = r0

    begin(fields.at[0])
    middle(1)

    def to_first(y, value):
        fields[1, y] = value

    finish(1, to_first)

    for sweep in range(SWEEPS):
        image = fields.at[sweep + 1]
        last = sweep + 1 == SWEEPS
        s1 = jnp.zeros((1, lanes), F32)
        s2, s3 = s1, s1
        for y in range(ny):
            f, r = image[y], res_ref[y]
            s1 = s1 + jnp.sum(f * r, axis=0, keepdims=True)
            s2 = s2 + jnp.sum(f * swap(r), axis=0, keepdims=True)
            s3 = s3 + jnp.sum(f * f, axis=0, keepdims=True)
        num = jnp.where(low, s1 + swap(s1), swap(s2) - s2)
        den = s3 + swap(s3)
        row = lax.broadcasted_iota(jnp.int32, (2, lanes), 0)
        tbuf, pbuf = at_buf.at[sweep], ap_buf.at[sweep]
        mine, n, peer = (rank, everyone, any_peer) if direct else (it, nt, time_peer)
        tbuf[mine] = jnp.where(row == 0, num, den)
        t_copies = share(tbuf, mine, n, peer, at_send.at[sweep], at_recv.at[sweep])
        sends += t_copies
        if not last:
            sends += send_field(sweep + 2, image)
            begin(image)
        if direct and not last:
            middle(sweep + 2)
        recv_all(t_copies)
        total = add_slots(tbuf, n)
        if not direct:
            pbuf[me] = total
            p_copies = share(pbuf, me, plane, plane_peer, ap_send.at[sweep], ap_recv.at[sweep])
            sends += p_copies
            if not last:
                middle(sweep + 2)
            recv_all(p_copies)
            total = add_slots(pbuf, plane)
        a = total[0:1] / total[1:2]
        sa = swap(a)
        ar = jnp.where(low, a, sa)
        ai = jnp.where(low, sa, a) * jsign
        for y in range(ny):
            f, r = image[y], res_ref[y]
            sol_ref[y] = sol_ref[y] + (ar * r + ai * swap(r))
            res_ref[y] = r - (ar * f + ai * swap(f))
        if not last:

            def update(y, value):
                fields[sweep + 2, y] = image[y] - (ar * value + ai * swap(value))

            finish(sweep + 2, update)
    for c in sends:
        c.wait_send()


def hand_over(a_ref, b_ref, sol_ref, res_ref):
    sol_ref[...] = a_ref[...]
    res_ref[...] = b_ref[...]


def local(sizes, links, eigvecs, eig_real, eig_imag, rhs):
    nt, nz, nx = sizes
    plane = nz * nx
    ny, dof, lanes = rhs.shape[3:]
    half = lanes // 2
    field = (ny, dof, lanes)
    ndir = links.shape[4]
    slots = sum(1 if n == 2 else 2 for n in sizes)
    part = half // plane
    rounds = SWEEPS + 1
    first = nt * plane if nt * plane <= DIRECT else nt
    vmem, dma = pltpu.VMEM, pltpu.SemaphoreType.DMA
    spec = pl.BlockSpec(memory_space=pltpu.VMEM)
    sol, res = pl.pallas_call(
        functools.partial(kernel, sizes, field),
        out_shape=[jax.ShapeDtypeStruct(field, F32)] * 2,
        in_specs=[pl.BlockSpec(memory_space=pl.ANY)] + [spec] * 4,
        out_specs=[spec] * 2,
        scratch_shapes=[
            vmem((ndir, ny, links.shape[5]), F32),
            vmem((ndir * ny * dof, 128), F32),
            vmem((ny, 3 * dof, (3 + slots) * 128), BF16),
            vmem((1 + slots, ny, 128, 3 * lanes), BF16),
            vmem(field, F32),
            vmem((rounds,) + field, F32),
            vmem((rounds, slots) + field, F32),
            vmem(field, F32),
            vmem((half, lanes), F32),
            vmem((plane, part, lanes), F32),
            vmem((plane, part, lanes), F32),
            vmem((nt, part, lanes), F32),
            vmem((plane, part, lanes), F32),
            vmem((SWEEPS, first, 2, lanes), F32),
            vmem((SWEEPS, plane, 2, lanes), F32),
            vmem((2 * ny * dof, 4 * lanes), BF16),
            dma,
            dma((rounds, slots)),
            dma((rounds, slots)),
            dma((plane,)),
            dma((plane,)),
            dma((nt,)),
            dma((nt,)),
            dma((plane,)),
            dma((plane,)),
            dma((SWEEPS, first)),
            dma((SWEEPS, first)),
            dma((SWEEPS, plane)),
            dma((SWEEPS, plane)),
        ],
        compiler_params=pltpu.CompilerParams(collective_id=0, has_side_effects=True),
    )(
        links.reshape(links.shape[3:]).transpose(1, 0, 2),
        eigvecs.reshape(field),
        eig_real.reshape(1, -1),
        eig_imag.reshape(1, -1),
        rhs.reshape(field),
    )
    sol, res = pl.pallas_call(
        hand_over,
        out_shape=[jax.ShapeDtypeStruct(field, F32)] * 2,
        in_specs=[spec] * 2,
        out_specs=[spec] * 2,
    )(sol, res)
    return (sol.reshape(rhs.shape), res.reshape(rhs.shape))


def solution(mesh):
    whole = P("ta", "gz", "xy", None, None, None)
    sizes = tuple(mesh.shape[a] for a in ("ta", "gz", "xy"))
    return jax.shard_map(
        functools.partial(local, sizes),
        mesh=mesh,
        in_specs=(whole, whole, P(), P(), whole),
        out_specs=(whole, whole),
        check_vma=False,
    )
```
